32 devices in a mesh: sp: 8 (over z, y), tp: 4 (over x, core).
Axes of the slice: x: 2, y: 2, z: 4, core: 2. Of those that a mesh axis runs over, the one named last changes fastest.
Arguments:
- decay_rate: float32 [4, 8192, 1024], P(None, 'sp', 'tp'), may hold values from 0.2 to 2
- drive_in: bfloat16 [4, 8192, 1024], P(None, 'sp', 'tp'), may hold values from -6 to 6
- gate_in: bfloat16 [4, 8192, 1024], P(None, 'sp', 'tp'), may hold values from -6 to 6
- norm_gain: float32 [1024], P('tp'), may hold values from 0.25 to 1.75
Outputs:
- filtered: bfloat16 [4, 8192, 1024], P(None, 'sp', 'tp')
The draws below stay inside these ranges and needn't reach their ends.
All inputs are finite; a program needn't handle non-finite values.
Results may differ from the reference program's by a relative error of at most 0.0015.
Values sent between devices are 32-bit elements.
A program may use at most 128 MiB of HBM per device.

```python
import jax
import jax.numpy as jnp
from jax import lax

BATCH = 4
CHANNELS = 1024
LENGTH = 8192


def block_scale(stream_key, extent, shards, smallest, high):
    def one(dim, blocks):
        steps = jax.random.uniform(jax.random.fold_in(jax.random.fold_in(stream_key, 6), dim), (blocks,), jnp.float32, smallest / len(shards), high / len(shards))
        return jnp.repeat(jnp.exp(steps), extent[dim] // blocks).reshape((-1,) + (1,) * (len(extent) - dim - 1))

    factor_of = one(*shards[0])
    for cut in shards[1:]:
        factor_of = factor_of * one(*cut)
    return factor_of


def gaussian(stream_key, dims, width, reach, pieces=(), held_as=jnp.bfloat16):
    array = jax.random.normal(stream_key, dims, jnp.float32) * width
    if len(pieces) > 0:
        array = block_scale(stream_key, dims, pieces, -0.22, 0.18) * array
    return jnp.clip(array, min=-reach, max=reach).astype(held_as)


def setup_inputs(seed: int = 0) -> dict:
    streams_of = jax.random.split(jax.random.key(seed), 5)
    decay_rate = jnp.clip(0.2 + 1.8 * jax.random.uniform(streams_of[0], (BATCH, LENGTH, CHANNELS), jnp.float32) ** block_scale(streams_of[0], (BATCH, LENGTH, CHANNELS), ((1, 8), (2, 4)), -0.2, 0.2), 0.2, 2.0)
    drive_in = gaussian(streams_of[1], (BATCH, LENGTH, CHANNELS), 1.0, 6.0, ((1, 8), (2, 4)))
    gate_in = gaussian(streams_of[2], (BATCH, LENGTH, CHANNELS), 1.0, 6.0, ((1, 8), (2, 4)))
    norm_gain = jnp.clip(1.0 + 0.15 * jax.random.normal(streams_of[3], (CHANNELS,), jnp.float32), 0.25, 1.75)
    return dict(decay_rate=decay_rate, drive_in=drive_in, gate_in=gate_in, norm_gain=norm_gain)


def join_pair(earlier, later):
    return (earlier[0] * later[0], later[0] * earlier[1] + later[1])

def reference(decay_rate, drive_in, gate_in, norm_gain):
    keep = jnp.exp(-decay_rate / LENGTH)
    push = drive_in.astype(jnp.float32) * LENGTH ** (-0.5)
    forward = lax.associative_scan(join_pair, (keep, push), axis=1)[1]
    gated = forward * jax.nn.sigmoid(gate_in.astype(jnp.float32))
    power = lax.optimization_barrier(jnp.mean(gated * gated, axis=-1, keepdims=True))
    filtered = (gated * lax.rsqrt(power + 1e-06) * norm_gain).astype(jnp.bfloat16)
    return filtered
```

```python
import functools

import jax
import jax.numpy as jnp
from jax import lax
from jax.experimental import pallas as pl
from jax.experimental.pallas import tpu as pltpu
from jax.sharding import PartitionSpec as P

CHUNK = 128
MESH = pl.DeviceIdType.MESH


def split(x):
    high = x.astype(jnp.bfloat16)
    low = (x - high.astype(jnp.float32)).astype(jnp.bfloat16)
    return jnp.concatenate([high, low], axis=0)


def kernel(
    n_sp, n_tp, total_length, decay_hbm, drive_hbm, gate_hbm, gain_ref, out_hbm,
    decay, drive, gate, sums, out, chunk_keep, chunk_state,
    mine, gathered, my_power, powers,
    in_sem, out_sem, sp_send, sp_recv, tp_send, tp_recv,
):
    batch, length, channels = decay.shape
    chunks = length // CHUNK
    sp, tp = lax.axis_index("sp"), lax.axis_index("tp")

    def load(b, which):
        src, dst = ((decay_hbm, decay), (drive_hbm, drive), (gate_hbm, gate))[which]
        return pltpu.make_async_copy(src.at[b], dst.at[b], in_sem.at[which, b])

    def store(b):
        return pltpu.make_async_copy(out.at[b], out_hbm.at[b], out_sem.at[b])

    def to_later(j, b):
        return pltpu.make_async_remote_copy(
            src_ref=mine.at[b], dst_ref=gathered.at[sp, b],
            send_sem=sp_send.at[j, b], recv_sem=sp_recv.at[sp, b],
            device_id={"sp": j}, device_id_type=MESH,
        )

    def from_earlier(j, b):
        return pltpu.make_async_remote_copy(
            src_ref=mine.at[b], dst_ref=gathered.at[j, b],
            send_sem=sp_send.at[j, b], recv_sem=sp_recv.at[j, b],
            device_id={"sp": j}, device_id_type=MESH,
        )

    def to_peer(i, b):
        return pltpu.make_async_remote_copy(
            src_ref=my_power.at[b], dst_ref=powers.at[i - 1, b],
            send_sem=tp_send.at[i - 1, b], recv_sem=tp_recv.at[i - 1, b],
            device_id={"tp": lax.rem(tp + i, n_tp)}, device_id_type=MESH,
        )

    for b in range(batch):
        load(b, 0).start()
        load(b, 1).start()
    for b in range(batch):
        load(b, 2).start()

    barrier = pltpu.get_barrier_semaphore()

    def greet(j, _):
        pl.semaphore_signal(barrier, inc=1, device_id={"sp": j}, device_id_type=MESH)
        return 0

    lax.fori_loop(0, sp, greet, 0)
    for i in range(1, n_tp):
        pl.semaphore_signal(
            barrier, inc=1, device_id={"tp": lax.rem(tp + i, n_tp)}, device_id_type=MESH
        )

    row = lax.broadcasted_iota(jnp.int32, (CHUNK, 2 * CHUNK), 0)
    column = lax.broadcasted_iota(jnp.int32, (CHUNK, 2 * CHUNK), 1)
    column = jnp.where(column >= CHUNK, column - CHUNK, column)
    lower = jnp.where(column <= row, 1.0, 0.0).astype(jnp.bfloat16)

    def running(x):
        return jnp.dot(lower, split(x), preferred_element_type=jnp.float32)

    def scan_batch(b, _):
        load(b, 0).wait()
        load(b, 1).wait()
        keep = jnp.ones((1, channels), jnp.float32)
        state = jnp.zeros((1, channels), jnp.float32)
        for k in range(chunks):
            at = pl.ds(k * CHUNK, CHUNK)
            passed = running(decay[b, at]) * (1.0 / total_length)
            summed = running(jnp.exp(passed) * drive[b, at].astype(jnp.float32))
            fall = jnp.exp(-passed)
            decay[b, at] = fall
            sums[b, at] = summed
            chunk_keep[b, pl.ds(k, 1)] = keep
            chunk_state[b, pl.ds(k, 1)] = state
            last = fall[CHUNK - 1 :]
            state = last * (state + summed[CHUNK - 1 :])
            keep = last * keep
        mine[b, pl.ds(0, 1)] = keep
        mine[b, pl.ds(1, 1)] = state

        @pl.when(b == 0)
        def _():
            pl.semaphore_wait(barrier, n_sp - 1 - sp + n_tp - 1)

        def send(i, _):
            to_later(n_sp - 1 - i, b).start()
            return 0

        lax.fori_loop(0, n_sp - 1 - sp, send, 0)
        return 0

    lax.fori_loop(0, batch, scan_batch, 0)

    def gate_batch(b, _):
        load(b, 2).wait()
        for k in range(chunks):
            at = pl.ds(k * CHUNK, CHUNK)
            opened = decay[b, at] * (1.0 + jnp.tanh(0.5 * gate[b, at].astype(jnp.float32)))
            decay[b, at] = opened
            sums[b, at] = opened * sums[b, at]
        return 0

    lax.fori_loop(0, batch, gate_batch, 0)

    lane = lax.broadcasted_iota(jnp.int32, (CHUNK, CHUNK), 1)

    def join_batch(b, _):
        def earlier(j, state):
            from_earlier(j, b).wait_recv()
            return gathered[j, b, pl.ds(0, 1)] * state + gathered[j, b, pl.ds(1, 1)]

        entering = lax.fori_loop(0, sp, earlier, jnp.zeros((1, channels), jnp.float32))
        states = chunk_keep[b] * entering + chunk_state[b]
        squares = jnp.zeros((CHUNK, CHUNK), jnp.float32)
        for k in range(chunks):
            at = pl.ds(k * CHUNK, CHUNK)
            gated = decay[b, at] * states[k : k + 1] + sums[b, at]
            sums[b, at] = gated
            squares = jnp.where(lane == k, jnp.sum(gated * gated, axis=1, keepdims=True), squares)
        my_power[b] = jnp.transpose(squares)[:chunks]
        for i in range(1, n_tp):
            to_peer(i, b).start()
        return 0

    lax.fori_loop(0, batch, join_batch, 0)

    gain = gain_ref[...]

    def norm_batch(b, _):
        power = my_power[b]
        for i in range(1, n_tp):
            to_peer(i, b).wait_recv()
            power = power + powers[i - 1, b]
        scale = lax.rsqrt(power / (channels * n_tp) + 4e-6 * total_length)
        scale = jnp.transpose(
            jnp.concatenate([scale, jnp.zeros((CHUNK - chunks, CHUNK), jnp.float32)], axis=0)
        )
        for k in range(chunks):
            at = pl.ds(k * CHUNK, CHUNK)
            out[b, at] = (sums[b, at] * scale[:, k : k + 1] * gain).astype(jnp.bfloat16)
        store(b).start()
        return 0

    lax.fori_loop(0, batch, norm_batch, 0)

    for b in range(batch):
        store(b).wait()

        def sent(i, _):
            to_later(n_sp - 1 - i, b).wait_send()
            return 0

        lax.fori_loop(0, n_sp - 1 - sp, sent, 0)
        for i in range(1, n_tp):
            to_peer(i, b).wait_send()


def solution(mesh):
    n_sp, n_tp = mesh.shape["sp"], mesh.shape["tp"]

    def shards(decay_rate, drive_in, gate_in, norm_gain):
        batch, length, channels = decay_rate.shape
        chunks = length // CHUNK
        f32 = jnp.float32
        return pl.pallas_call(
            functools.partial(kernel, n_sp, n_tp, length * n_sp),
            out_shape=jax.ShapeDtypeStruct((batch, length, channels), jnp.bfloat16),
            in_specs=[pl.BlockSpec(memory_space=pl.ANY)] * 3
            + [pl.BlockSpec(memory_space=pltpu.VMEM)],
            out_specs=pl.BlockSpec(memory_space=pl.ANY),
            scratch_shapes=[
                pltpu.VMEM((batch, length, channels), f32),
                pltpu.VMEM((batch, length, channels), jnp.bfloat16),
                pltpu.VMEM((batch, length, channels), jnp.bfloat16),
                pltpu.VMEM((batch, length, channels), f32),
                pltpu.VMEM((batch, length, channels), jnp.bfloat16),
                pltpu.VMEM((batch, chunks, channels), f32),
                pltpu.VMEM((batch, chunks, channels), f32),
                pltpu.VMEM((batch, 2, channels), f32),
                pltpu.VMEM((n_sp, batch, 2, channels), f32),
                pltpu.VMEM((batch, chunks, CHUNK), f32),
                pltpu.VMEM((n_tp - 1, batch, chunks, CHUNK), f32),
                pltpu.SemaphoreType.DMA((3, batch)),
                pltpu.SemaphoreType.DMA((batch,)),
                pltpu.SemaphoreType.DMA((n_sp, batch)),
                pltpu.SemaphoreType.DMA((n_sp, batch)),
                pltpu.SemaphoreType.DMA((n_tp - 1, batch)),
                pltpu.SemaphoreType.DMA((n_tp - 1, batch)),
            ],
            compiler_params=pltpu.CompilerParams(collective_id=0, has_side_effects=True),
        )(decay_rate, drive_in, gate_in, norm_gain.reshape(1, channels))

    placed = (P(None, "sp", "tp"), P(None, "sp", "tp"), P(None, "sp", "tp"), P("tp"))
    return jax.shard_map(
        shards, mesh=mesh, in_specs=placed, out_specs=P(None, "sp", "tp"), check_vma=False
    )
```

```python
import functools

import jax
import jax.numpy as jnp
from jax import lax
from jax.experimental import pallas as pl
from jax.experimental.pallas import tpu as pltpu
from jax.sharding import PartitionSpec as P

CHUNK = 128
MESH = pl.DeviceIdType.MESH


def split(x):
    high = x.astype(jnp.bfloat16)
    low = (x - high.astype(jnp.float32)).astype(jnp.bfloat16)
    return jnp.concatenate([high, low], axis=0)


def kernel(
    n_sp, n_tp, total_length, decay_hbm, drive_hbm, gate_hbm, gain_hbm, out,
    decay, drive, gate, gain_ref, sums, chunk_keep, chunk_state,
    mine, gathered, my_power, powers,
    in_sem, gain_sem, sp_send, sp_recv, tp_send, tp_recv,
):
    batch, length, channels = decay.shape
    chunks = length // CHUNK
    sp, tp = lax.axis_index("sp"), lax.axis_index("tp")

    def load(b, which):
        src, dst = ((decay_hbm, decay), (drive_hbm, drive), (gate_hbm, gate))[which]
        return pltpu.make_async_copy(src.at[b], dst.at[b], in_sem.at[which, b])

    def to_later(j, b):
        return pltpu.make_async_remote_copy(
            src_ref=mine.at[b], dst_ref=gathered.at[sp, b],
            send_sem=sp_send.at[j, b], recv_sem=sp_recv.at[sp, b],
            device_id={"sp": j}, device_id_type=MESH,
        )

    def from_earlier(j, b):
        return pltpu.make_async_remote_copy(
            src_ref=mine.at[b], dst_ref=gathered.at[j, b],
            send_sem=sp_send.at[j, b], recv_sem=sp_recv.at[j, b],
            device_id={"sp": j}, device_id_type=MESH,
        )

    def to_peer(i, b):
        return pltpu.make_async_remote_copy(
            src_ref=my_power.at[b], dst_ref=powers.at[i - 1, b],
            send_sem=tp_send.at[i - 1, b], recv_sem=tp_recv.at[i - 1, b],
            device_id={"tp": lax.rem(tp + i, n_tp)}, device_id_type=MESH,
        )

    for b in range(batch):
        load(b, 0).start()
        load(b, 1).start()
    for b in range(batch):
        load(b, 2).start()
    gain_load = pltpu.make_async_copy(gain_hbm, gain_ref, gain_sem)
    gain_load.start()

    barrier = pltpu.get_barrier_semaphore()

    def greet(j, _):
        pl.semaphore_signal(barrier, inc=1, device_id={"sp": j}, device_id_type=MESH)
        return 0

    lax.fori_loop(0, sp, greet, 0)
    for i in range(1, n_tp):
        pl.semaphore_signal(
            barrier, inc=1, device_id={"tp": lax.rem(tp + i, n_tp)}, device_id_type=MESH
        )

    row = lax.broadcasted_iota(jnp.int32, (CHUNK, 2 * CHUNK), 0)
    column = lax.broadcasted_iota(jnp.int32, (CHUNK, 2 * CHUNK), 1)
    column = jnp.where(column >= CHUNK, column - CHUNK, column)
    lower = jnp.where(column <= row, 1.0, 0.0).astype(jnp.bfloat16)

    def running(x):
        return jnp.dot(lower, split(x), preferred_element_type=jnp.float32)

    def scan_batch(b, _):
        load(b, 0).wait()
        load(b, 1).wait()
        keep = jnp.ones((1, channels), jnp.float32)
        state = jnp.zeros((1, channels), jnp.float32)
        for k in range(chunks):
            at = pl.ds(k * CHUNK, CHUNK)
            passed = running(decay[b, at]) * (1.0 / total_length)
            summed = running(jnp.exp(passed) * drive[b, at].astype(jnp.float32))
            fall = jnp.exp(-passed)
            decay[b, at] = fall
            sums[b, at] = summed
            chunk_keep[b, pl.ds(k, 1)] = keep
            chunk_state[b, pl.ds(k, 1)] = state
            last = fall[CHUNK - 1 :]
            state = last * (state + summed[CHUNK - 1 :])
            keep = last * keep
        mine[b, pl.ds(0, 1)] = keep
        mine[b, pl.ds(1, 1)] = state

        @pl.when(b == 0)
        def _():
            pl.semaphore_wait(barrier, n_sp - 1 - sp + n_tp - 1)

        def send(i, _):
            to_later(n_sp - 1 - i, b).start()
            return 0

        lax.fori_loop(0, n_sp - 1 - sp, send, 0)
        return 0

    lax.fori_loop(0, batch, scan_batch, 0)

    def gate_batch(b, _):
        load(b, 2).wait()
        for k in range(chunks):
            at = pl.ds(k * CHUNK, CHUNK)
            opened = decay[b, at] * (1.0 + jnp.tanh(0.5 * gate[b, at].astype(jnp.float32)))
            decay[b, at] = opened
            sums[b, at] = opened * sums[b, at]
        return 0

    lax.fori_loop(0, batch, gate_batch, 0)

    lane = lax.broadcasted_iota(jnp.int32, (CHUNK, CHUNK), 1)

    def join_batch(b, _):
        def earlier(j, state):
            from_earlier(j, b).wait_recv()
            return gathered[j, b, pl.ds(0, 1)] * state + gathered[j, b, pl.ds(1, 1)]

        entering = lax.fori_loop(0, sp, earlier, jnp.zeros((1, channels), jnp.float32))
        states = chunk_keep[b] * entering + chunk_state[b]
        squares = jnp.zeros((CHUNK, CHUNK), jnp.float32)
        for k in range(chunks):
            at = pl.ds(k * CHUNK, CHUNK)
            gated = decay[b, at] * states[k : k + 1] + sums[b, at]
            sums[b, at] = gated
            squares = jnp.where(lane == k, jnp.sum(gated * gated, axis=1, keepdims=True), squares)
        my_power[b] = jnp.transpose(squares)[:chunks]
        for i in range(1, n_tp):
            to_peer(i, b).start()
        return 0

    lax.fori_loop(0, batch, join_batch, 0)

    gain_load.wait()
    gain = gain_ref[...]

    def norm_batch(b, _):
        power = my_power[b]
        for i in range(1, n_tp):
            to_peer(i, b).wait_recv()
            power = power + powers[i - 1, b]
        scale = lax.rsqrt(power / (channels * n_tp) + 4e-6 * total_length)
        scale = jnp.transpose(
            jnp.concatenate([scale, jnp.zeros((CHUNK - chunks, CHUNK), jnp.float32)], axis=0)
        )
        for k in range(chunks):
            at = pl.ds(k * CHUNK, CHUNK)
            out[b, at] = (sums[b, at] * scale[:, k : k + 1] * gain).astype(jnp.bfloat16)
        return 0

    lax.fori_loop(0, batch, norm_batch, 0)

    for b in range(batch):
        def sent(i, _):
            to_later(n_sp - 1 - i, b).wait_send()
            return 0

        lax.fori_loop(0, n_sp - 1 - sp, sent, 0)
        for i in range(1, n_tp):
            to_peer(i, b).wait_send()


def put_kernel(held, out_hbm, sem):
    copies = [
        pltpu.make_async_copy(held.at[b], out_hbm.at[b], sem.at[b]) for b in range(held.shape[0])
    ]
    for copy in copies:
        copy.start()
    for copy in copies:
        copy.wait()


def solution(mesh):
    n_sp, n_tp = mesh.shape["sp"], mesh.shape["tp"]

    def shards(decay_rate, drive_in, gate_in, norm_gain):
        batch, length, channels = decay_rate.shape
        chunks = length // CHUNK
        f32 = jnp.float32
        held = pl.pallas_call(
            functools.partial(kernel, n_sp, n_tp, length * n_sp),
            out_shape=pltpu.VMEM((batch, length, channels), jnp.bfloat16),
            in_specs=[pl.BlockSpec(memory_space=pltpu.HBM)] * 4,
            out_specs=pl.BlockSpec(memory_space=pltpu.VMEM),
            scratch_shapes=[
                pltpu.VMEM((batch, length, channels), f32),
                pltpu.VMEM((batch, length, channels), jnp.bfloat16),
                pltpu.VMEM((batch, length, channels), jnp.bfloat16),
                pltpu.VMEM((1, channels), f32),
                pltpu.VMEM((batch, length, channels), f32),
                pltpu.VMEM((batch, chunks, channels), f32),
                pltpu.VMEM((batch, chunks, channels), f32),
                pltpu.VMEM((batch, 2, channels), f32),
                pltpu.VMEM((n_sp, batch, 2, channels), f32),
                pltpu.VMEM((batch, chunks, CHUNK), f32),
                pltpu.VMEM((n_tp - 1, batch, chunks, CHUNK), f32),
                pltpu.SemaphoreType.DMA((3, batch)),
                pltpu.SemaphoreType.DMA,
                pltpu.SemaphoreType.DMA((n_sp, batch)),
                pltpu.SemaphoreType.DMA((n_sp, batch)),
                pltpu.SemaphoreType.DMA((n_tp - 1, batch)),
                pltpu.SemaphoreType.DMA((n_tp - 1, batch)),
            ],
            compiler_params=pltpu.CompilerParams(collective_id=0, has_side_effects=True),
        )(decay_rate, drive_in, gate_in, norm_gain.reshape(1, channels))
        return pl.pallas_call(
            put_kernel,
            out_shape=jax.ShapeDtypeStruct(held.shape, held.dtype),
            in_specs=[pl.BlockSpec(memory_space=pl.ANY)],
            out_specs=pl.BlockSpec(memory_space=pltpu.HBM),
            scratch_shapes=[pltpu.SemaphoreType.DMA((batch,))],
            compiler_params=pltpu.CompilerParams(vmem_limit_bytes=4 * 2**20),
        )(held)

    placed = (P(None, "sp", "tp"), P(None, "sp", "tp"), P(None, "sp", "tp"), P("tp"))
    return jax.shard_map(
        shards, mesh=mesh, in_specs=placed, out_specs=P(None, "sp", "tp"), check_vma=False
    )
```

```python
import functools

import jax
import jax.numpy as jnp
from jax import lax
from jax.experimental import pallas as pl
from jax.experimental.pallas import tpu as pltpu
from jax.sharding import PartitionSpec as P

CHUNK = 128
MESH = pl.DeviceIdType.MESH


def split(x):
    high = x.astype(jnp.bfloat16)
    low = (x - high.astype(jnp.float32)).astype(jnp.bfloat16)
    return jnp.concatenate([high, low], axis=0)


def kernel(
    n_sp, n_tp, total_length, decay_hbm, drive_hbm, gate_hbm, gain_hbm, out,
    decay, drive, gate, gain_ref, sums, chunk_keep, chunk_state,
    mine, gathered, my_power, powers,
    in_sem, gain_sem, sp_send, sp_recv, tp_send, tp_recv,
):
    batch, length, channels = decay.shape
    chunks = length // CHUNK
    sp, tp = lax.axis_index("sp"), lax.axis_index("tp")

    def load(b, which):
        src, dst = ((decay_hbm, decay), (drive_hbm, drive), (gate_hbm, gate))[which]
        return pltpu.make_async_copy(src.at[b], dst.at[b], in_sem.at[which, b])

    def to_later(j, b):
        return pltpu.make_async_remote_copy(
            src_ref=mine.at[b], dst_ref=gathered.at[sp, b],
            send_sem=sp_send.at[j, b], recv_sem=sp_recv.at[sp, b],
            device_id={"sp": j}, device_id_type=MESH,
        )

    def from_earlier(j, b):
        return pltpu.make_async_remote_copy(
            src_ref=mine.at[b], dst_ref=gathered.at[j, b],
            send_sem=sp_send.at[j, b], recv_sem=sp_recv.at[j, b],
            device_id={"sp": j}, device_id_type=MESH,
        )

    def to_peer(i, b):
        return pltpu.make_async_remote_copy(
            src_ref=my_power.at[b], dst_ref=powers.at[i - 1, b],
            send_sem=tp_send.at[i - 1, b], recv_sem=tp_recv.at[i - 1, b],
            device_id={"tp": lax.rem(tp + i, n_tp)}, device_id_type=MESH,
        )

    for b in range(batch):
        load(b, 0).start()
        load(b, 1).start()
    for b in range(batch):
        load(b, 2).start()
    gain_load = pltpu.make_async_copy(gain_hbm, gain_ref, gain_sem)
    gain_load.start()

    barrier = pltpu.get_barrier_semaphore()

    def greet(j, _):
        pl.semaphore_signal(barrier, inc=1, device_id={"sp": j}, device_id_type=MESH)
        return 0

    lax.fori_loop(0, sp, greet, 0)
    for i in range(1, n_tp):
        pl.semaphore_signal(
            barrier, inc=1, device_id={"tp": lax.rem(tp + i, n_tp)}, device_id_type=MESH
        )

    row = lax.broadcasted_iota(jnp.int32, (CHUNK, 2 * CHUNK), 0)
    column = lax.broadcasted_iota(jnp.int32, (CHUNK, 2 * CHUNK), 1)
    column = jnp.where(column >= CHUNK, column - CHUNK, column)
    lower = jnp.where(column <= row, 1.0, 0.0).astype(jnp.bfloat16)

    def running(x):
        return jnp.dot(lower, split(x), preferred_element_type=jnp.float32)

    def scan_batch(b, _):
        load(b, 0).wait()
        load(b, 1).wait()
        keep = jnp.ones((1, channels), jnp.float32)
        state = jnp.zeros((1, channels), jnp.float32)
        for k in range(chunks):
            at = pl.ds(k * CHUNK, CHUNK)
            passed = running(decay[b, at]) * (1.0 / total_length)
            pushed = jnp.exp(passed) * drive[b, at].astype(jnp.float32)
            fall = jnp.exp(-passed)
            decay[b, at] = fall
            sums[b, at] = pushed
            chunk_keep[b, pl.ds(k, 1)] = keep
            chunk_state[b, pl.ds(k, 1)] = state
            last = fall[CHUNK - 1 :]
            state = last * (state + jnp.sum(pushed, axis=0, keepdims=True))
            keep = last * keep
        mine[b, pl.ds(0, 1)] = keep
        mine[b, pl.ds(1, 1)] = state

        @pl.when(b == 0)
        def _():
            pl.semaphore_wait(barrier, n_sp - 1 - sp + n_tp - 1)

        def send(i, _):
            to_later(n_sp - 1 - i, b).start()
            return 0

        lax.fori_loop(0, n_sp - 1 - sp, send, 0)
        return 0

    lax.fori_loop(0, batch, scan_batch, 0)

    def gate_batch(b, _):
        load(b, 2).wait()
        for k in range(chunks):
            at = pl.ds(k * CHUNK, CHUNK)
            opened = decay[b, at] * (1.0 + jnp.tanh(0.5 * gate[b, at].astype(jnp.float32)))
            decay[b, at] = opened
            sums[b, at] = opened * running(sums[b, at])
        return 0

    lax.fori_loop(0, batch, gate_batch, 0)

    lane = lax.broadcasted_iota(jnp.int32, (CHUNK, CHUNK), 1)

    def join_batch(b, _):
        def earlier(j, state):
            from_earlier(j, b).wait_recv()
            return gathered[j, b, pl.ds(0, 1)] * state + gathered[j, b, pl.ds(1, 1)]

        entering = lax.fori_loop(0, sp, earlier, jnp.zeros((1, channels), jnp.float32))
        states = chunk_keep[b] * entering + chunk_state[b]
        squares = jnp.zeros((CHUNK, CHUNK), jnp.float32)
        for k in range(chunks):
            at = pl.ds(k * CHUNK, CHUNK)
            gated = decay[b, at] * states[k : k + 1] + sums[b, at]
            sums[b, at] = gated
            squares = jnp.where(lane == k, jnp.sum(gated * gated, axis=1, keepdims=True), squares)
        my_power[b] = jnp.transpose(squares)[:chunks]
        for i in range(1, n_tp):
            to_peer(i, b).start()
        return 0

    lax.fori_loop(0, batch, join_batch, 0)

    gain_load.wait()
    gain = gain_ref[...]

    def norm_batch(b, _):
        power = my_power[b]
        for i in range(1, n_tp):
            to_peer(i, b).wait_recv()
            power = power + powers[i - 1, b]
        scale = lax.rsqrt(power / (channels * n_tp) + 4e-6 * total_length)
        scale = jnp.transpose(
            jnp.concatenate([scale, jnp.zeros((CHUNK - chunks, CHUNK), jnp.float32)], axis=0)
        )
        for k in range(chunks):
            at = pl.ds(k * CHUNK, CHUNK)
            out[b, at] = (sums[b, at] * scale[:, k : k + 1] * gain).astype(jnp.bfloat16)
        return 0

    lax.fori_loop(0, batch, norm_batch, 0)

    for b in range(batch):
        def sent(i, _):
            to_later(n_sp - 1 - i, b).wait_send()
            return 0

        lax.fori_loop(0, n_sp - 1 - sp, sent, 0)
        for i in range(1, n_tp):
            to_peer(i, b).wait_send()


def put_kernel(held, out_hbm, sem):
    copies = [
        pltpu.make_async_copy(held.at[b], out_hbm.at[b], sem.at[b]) for b in range(held.shape[0])
    ]
    for copy in copies:
        copy.start()
    for copy in copies:
        copy.wait()


def solution(mesh):
    n_sp, n_tp = mesh.shape["sp"], mesh.shape["tp"]

    def shards(decay_rate, drive_in, gate_in, norm_gain):
        batch, length, channels = decay_rate.shape
        chunks = length // CHUNK
        f32 = jnp.float32
        held = pl.pallas_call(
            functools.partial(kernel, n_sp, n_tp, length * n_sp),
            out_shape=pltpu.VMEM((batch, length, channels), jnp.bfloat16),
            in_specs=[pl.BlockSpec(memory_space=pltpu.HBM)] * 4,
            out_specs=pl.BlockSpec(memory_space=pltpu.VMEM),
            scratch_shapes=[
                pltpu.VMEM((batch, length, channels), f32),
                pltpu.VMEM((batch, length, channels), jnp.bfloat16),
                pltpu.VMEM((batch, length, channels), jnp.bfloat16),
                pltpu.VMEM((1, channels), f32),
                pltpu.VMEM((batch, length, channels), f32),
                pltpu.VMEM((batch, chunks, channels), f32),
                pltpu.VMEM((batch, chunks, channels), f32),
                pltpu.VMEM((batch, 2, channels), f32),
                pltpu.VMEM((n_sp, batch, 2, channels), f32),
                pltpu.VMEM((batch, chunks, CHUNK), f32),
                pltpu.VMEM((n_tp - 1, batch, chunks, CHUNK), f32),
                pltpu.SemaphoreType.DMA((3, batch)),
                pltpu.SemaphoreType.DMA,
                pltpu.SemaphoreType.DMA((n_sp, batch)),
                pltpu.SemaphoreType.DMA((n_sp, batch)),
                pltpu.SemaphoreType.DMA((n_tp - 1, batch)),
                pltpu.SemaphoreType.DMA((n_tp - 1, batch)),
            ],
            compiler_params=pltpu.CompilerParams(collective_id=0, has_side_effects=True),
        )(decay_rate, drive_in, gate_in, norm_gain.reshape(1, channels))
        return pl.pallas_call(
            put_kernel,
            out_shape=jax.ShapeDtypeStruct(held.shape, held.dtype),
            in_specs=[pl.BlockSpec(memory_space=pl.ANY)],
            out_specs=pl.BlockSpec(memory_space=pltpu.HBM),
            scratch_shapes=[pltpu.SemaphoreType.DMA((batch,))],
            compiler_params=pltpu.CompilerParams(vmem_limit_bytes=4 * 2**20),
        )(held)

    placed = (P(None, "sp", "tp"), P(None, "sp", "tp"), P(None, "sp", "tp"), P("tp"))
    return jax.shard_map(
        shards, mesh=mesh, in_specs=placed, out_specs=P(None, "sp", "tp"), check_vma=False
    )
```
